32 devices in a mesh: dom: 16 (over z, y, x), sub: 2 (over core).
Axes of the slice: x: 2, y: 2, z: 4, core: 2. Of those that a mesh axis runs over, the one named last changes fastest.
Arguments:
- right_side: float32 [8, 32, 128], P(None, ('dom', 'sub')), may hold values from -18 to 18
- matrix_blocks: float32 [32, 27, 128, 128], P(('dom', 'sub')), may hold values from -1 to 2
- block_cols: int32 [32, 27], P(('dom', 'sub')), may hold values from 0 to 31, as said below
- signs: int32 [32, 128], P(('dom', 'sub')), may hold values from 0 to 1
- sample_rows: int32 [4096], replicated, may hold values from 0 to 4095, as said below
Outputs:
- solution: float32 [8, 32, 128], P(None, ('dom', 'sub'))
- residual: float32 [8, 32, 128], P(None, ('dom', 'sub'))
- basis: float32 [5, 8, 32, 128], P(None, None, ('dom', 'sub'))
The draws below stay inside these ranges and needn't reach their ends.
Inputs may be any that keep to these rules, and one draw needn't show every extreme that they name: `block_cols`: slot 0 of every block row names the row itself; slot 1 names the row 1 before it (the row 1 after it in the first 1 row) and slot 2 the row 1 after it (the row 1 before it in the last 1 row); every other column lies in the block rows of the row's own device or of the device just before or just after it in the order of dom and sub; a column may repeat within a row. `sample_rows`: all distinct.
All inputs are finite; a program needn't handle non-finite values.
Results may differ from the reference program's by a relative error of at most 0.0003.
Values sent between devices are 32-bit elements; how exact they have to be, the bound alone decides.
A program may use at most 64 MiB of HBM per device.

```python
import math
import jax
import jax.numpy as jnp
from jax import lax

BS = 128
RB = 1
NNZ = 27
NRHS = 8
ITERS = 5
WINDOW = 4
SKETCH = 4096
NBR = 32


def draw_right_side(key, part):
    shape = (NRHS, NBR, BS)
    place = jnp.arange(NBR, dtype=jnp.float32) / max(NBR - 1, 1)
    noise = jnp.clip(jax.random.normal(key, shape, jnp.float32), -6.0, 6.0)
    scale = 1.0 + 2.0 * place
    return (noise * scale[None, :, None]).astype(jnp.float32)


def draw_block_cols(key, part):
    row_ids = jnp.arange(NBR, dtype=jnp.int32)
    before = jnp.where(row_ids >= RB, row_ids - RB, row_ids + RB)
    after = jnp.where(row_ids + RB < NBR, row_ids + RB, row_ids - RB)
    offsets = jax.random.randint(key, (NBR, NNZ - 3), 0, 3 * RB, dtype=jnp.int32)
    base = (row_ids // RB - 1) * RB
    columns = base[:, None] + offsets
    columns = jnp.where(columns < 0, columns + RB, columns)
    columns = jnp.where(columns >= NBR, columns - RB, columns)
    return jnp.concatenate([row_ids[:, None], before[:, None], after[:, None], columns], axis=1).astype(jnp.int32)


def draw_matrix_blocks(key, part):
    spread = 0.6 / math.sqrt(NNZ * BS)
    shape = (NBR, NNZ, BS, BS)
    noise = jnp.clip(jax.random.normal(key, shape, jnp.float32), -6.0, 6.0) * spread
    slot_zero = (jnp.arange(NNZ) == 0).astype(jnp.float32)
    identity = jnp.eye(BS, dtype=jnp.float32)
    return (noise + slot_zero[None, :, None, None] * identity[None, None]).astype(jnp.float32)


def draw_sample_rows(key, part):
    order = jax.random.permutation(jax.random.fold_in(key, 7), NBR * BS)
    return order[:SKETCH].astype(jnp.int32)


def place_ends(array, key, smallest, largest):
    spot = [jax.random.randint(jax.random.fold_in(key, axis), (), 0, length) for axis, length in enumerate(array.shape)]
    longest = array.shape.index(max(array.shape))
    next_to = spot[:longest] + [(spot[longest] + 1) % array.shape[longest]] + spot[longest + 1:]
    return array.at[tuple(spot)].set(smallest).at[tuple(next_to)].set(largest)


def setup_inputs(seed: int = 0) -> dict:
    key_list = jax.random.split(jax.random.key(seed), 6)
    return {
        "right_side": draw_right_side(jax.random.fold_in(key_list[5], 71), 0),
        "matrix_blocks": draw_matrix_blocks(jax.random.fold_in(key_list[5], 71), 0),
        "block_cols": draw_block_cols(jax.random.fold_in(key_list[5], 71), 0),
        "signs": place_ends(jax.random.randint(key_list[3], (NBR, BS), 0, 2), jax.random.fold_in(key_list[3], 1), 0, 1).astype(jnp.int32),
        "sample_rows": draw_sample_rows(jax.random.fold_in(key_list[5], 71), 0),
    }


def dct_table():
    freq = jnp.arange(BS, dtype=jnp.float32)[:, None]
    place = jnp.arange(BS, dtype=jnp.float32)[None, :]
    table = jnp.sqrt(2.0 / BS) * jnp.cos(math.pi * (2.0 * place + 1.0) * freq / (2.0 * BS))
    factor = jnp.where(freq == 0.0, math.sqrt(0.5), 1.0).astype(jnp.float32)
    return (table * factor).astype(jnp.float32)

def multiply(matrix_blocks, block_cols, vectors):
    gathered = vectors[:, block_cols, :]
    return jnp.einsum('rkab,nrkb->nra', matrix_blocks, gathered, precision=lax.Precision.HIGHEST)

def sketch(vectors, signs, sample_rows, table):
    flipped = vectors * (2 * signs - 1).astype(jnp.float32)[None]
    mixed = jnp.einsum('ka,nra->nrk', table, flipped, precision=lax.Precision.HIGHEST)
    flat = mixed.reshape(NRHS, NBR * BS)
    return flat[:, sample_rows]

def solve_small(gram, load):
    factor = jnp.linalg.cholesky(gram)
    return jax.scipy.linalg.cho_solve((factor, True), load)

def reference(right_side, matrix_blocks, block_cols, signs, sample_rows):
    table = dct_table()
    beta = jnp.sqrt(lax.optimization_barrier(jnp.sum(right_side * right_side, axis=(1, 2))))
    basis = [right_side / beta[:, None, None]]
    images = []
    for column in range(ITERS):
        image = multiply(matrix_blocks, block_cols, basis[column])
        images.append(image)
        if column < ITERS - 1:
            window = jnp.stack(basis[max(0, column - WINDOW + 1):column + 1])
            coeffs = jnp.einsum('knrb,nrb->nk', window, image, precision=lax.Precision.HIGHEST)
            ortho = image - jnp.einsum('nk,knrb->nrb', coeffs, window, precision=lax.Precision.HIGHEST)
            length = jnp.sqrt(lax.optimization_barrier(jnp.sum(ortho * ortho, axis=(1, 2))))
            basis.append(ortho / length[:, None, None])
    target = sketch(right_side, signs, sample_rows, table)
    columns = jnp.stack([sketch(image, signs, sample_rows, table) for image in images])
    gram = jnp.einsum('inm,jnm->nij', columns, columns, precision=lax.Precision.HIGHEST)
    load = jnp.einsum('inm,nm->ni', columns, target, precision=lax.Precision.HIGHEST)
    coef = jax.vmap(solve_small)(gram, load)
    stacked = jnp.stack(basis)
    solution = jnp.einsum('nj,jnrb->nrb', coef, stacked, precision=lax.Precision.HIGHEST)
    residual = right_side - jnp.einsum('nj,jnrb->nrb', coef, jnp.stack(images), precision=lax.Precision.HIGHEST)
    scaled = stacked * jnp.float32(math.sqrt(NBR * BS))
    return (solution, residual, scaled)
```

```python
import functools
import math

import jax
import jax.numpy as jnp
import numpy as np
from jax import lax
from jax.experimental import pallas as pl
from jax.experimental.pallas import tpu as pltpu
from jax.sharding import PartitionSpec as P

ITERS = 5
WINDOW = 4
MESH = pl.DeviceIdType.MESH


def dct_table(block_size):
    freq = np.arange(block_size, dtype=np.float64)[:, None]
    place = np.arange(block_size, dtype=np.float64)[None, :]
    table = np.sqrt(2.0 / block_size) * np.cos(
        math.pi * (2.0 * place + 1.0) * freq / (2.0 * block_size)
    )
    factor = np.where(freq == 0.0, math.sqrt(0.5), 1.0)
    return (table * factor).astype(np.float32)


PARTS = 3


def split(value):
    pieces = []
    for _ in range(PARTS):
        rounded = value.astype(jnp.bfloat16).astype(jnp.float32)
        pieces.append(rounded)
        value = value - rounded
    return pieces


def dot_split(left, right):
    rows = left.shape[0]
    width = right.shape[0] // PARTS
    tall = jnp.concatenate(split(left), axis=0).astype(jnp.bfloat16)
    out = lax.dot_general(
        tall, right, (((1,), (1,)), ((), ())), preferred_element_type=jnp.float32
    )
    total = None
    for i in reversed(range(PARTS)):
        for k in reversed(range(PARTS - i)):
            term = out[i * rows : (i + 1) * rows, k * width : (k + 1) * width]
            total = term if total is None else total + term
    return total


def kernel(
    ndev, nsub, order_total,
    b_hbm, m_ref, cols_ref, signs_hbm, rows_hbm, table_hbm,
    out_ref,
    b_ref, signs_ref, rows_ref, table_ref,
    slots, near, own, sides, sketch, sends, heard, gathered,
    load_sem, small_sem, xsend_sem, xrecv_sem, gsend_sem, grecv_sem,
):
    nrhs, width = b_hbm.shape
    nnz = m_ref.shape[0]
    quant = width // nrhs
    me = lax.axis_index("dom") * nsub + lax.axis_index("sub")

    def place(target):
        return (target // nsub, lax.rem(target, nsub))

    barrier = pltpu.get_barrier_semaphore()

    def greet(step, carry):
        target = lax.rem(me + step, ndev)
        pl.semaphore_signal(barrier, inc=1, device_id=place(target), device_id_type=MESH)
        return carry

    lax.fori_loop(1, ndev, greet, 0, unroll=ndev <= 64)

    smalls = [
        pltpu.make_async_copy(src, dst, small_sem.at[i])
        for i, (src, dst) in enumerate(
            [(rows_hbm, rows_ref), (signs_hbm, signs_ref), (table_hbm, table_ref), (b_hbm, b_ref)]
        )
    ]
    for copy in smalls:
        copy.start()
    pieces = 3
    bounds = [nnz * p // pieces for p in range(pieces + 1)]

    def piece(p):
        span = pl.ds(bounds[p], bounds[p + 1] - bounds[p])
        return pltpu.make_async_copy(m_ref.at[span], slots.at[span], load_sem.at[p])

    for p in range(pieces):
        piece(p).start()

    @pl.when(me == 0)
    def _():
        for step in range(ITERS):
            heard[step, 0] = jnp.zeros((nrhs, width), jnp.float32)

    @pl.when(me == ndev - 1)
    def _():
        for step in range(ITERS):
            heard[step, 1] = jnp.zeros((nrhs, width), jnp.float32)

    lane = lax.broadcasted_iota(jnp.int32, (nrhs, width), 1)
    sub_id = lax.broadcasted_iota(jnp.int32, (nrhs, width), 0)

    for copy in smalls:
        copy.wait()
    wanted = me * width + lax.broadcasted_iota(jnp.int32, (8, width), 1)
    listed = rows_hbm.shape[0]
    hit = jnp.zeros((8, width), jnp.int32)
    for top in range(0, listed, 8):
        values = rows_ref[pl.ds(top, 8), :]
        for shift in range(width):
            turned = values if shift == 0 else pltpu.roll(values, shift, 1)
            hit = jnp.where(turned == wanted, 1, hit)
    kept = jnp.max(hit, axis=0, keepdims=True).astype(jnp.float32)
    flips = (2 * signs_ref[...] - 1).astype(jnp.float32)
    eye = (
        lax.broadcasted_iota(jnp.int32, (width, width), 0)
        == lax.broadcasted_iota(jnp.int32, (width, width), 1)
    )
    kept_col = jnp.sum(jnp.where(eye, kept, 0.0), axis=1, keepdims=True)
    for i, part in enumerate(split(table_ref[...] * flips * kept_col)):
        sketch[pl.ds(i * width, width), :] = part.astype(jnp.bfloat16)

    half = width // 2
    for p in range(pieces):
        piece(p).wait()
        for part in range(2):
            span = pl.ds(part * half, half)
            if p == 0:
                sums = [jnp.zeros((half, width), jnp.float32) for _ in range(3)]
            else:
                sums = [near[d, span, :] for d in range(3)]
            for slot in range(bounds[p], bounds[p + 1]):
                block = slots[slot, span, :]
                offset = cols_ref[0, slot] - me + 1
                for d in range(3):
                    share = jnp.where(offset == d, 1.0, 0.0).astype(jnp.float32)
                    sums[d] = sums[d] + share * block
            for d in range(3):
                near[d, span, :] = sums[d]

    for d, target, first in ((1, own, 0), (0, sides, 0), (2, sides, width)):
        for i, part in enumerate(split(near[d])):
            target[pl.ds(i * width, width), pl.ds(first, width)] = part.astype(jnp.bfloat16)

    pl.semaphore_wait(barrier, ndev - 1)

    def copy_to(step, side):
        target = me + 1 if side == 0 else me - 1
        return pltpu.make_async_remote_copy(
            src_ref=sends.at[step], dst_ref=heard.at[step, side],
            send_sem=xsend_sem.at[step, side], recv_sem=xrecv_sem.at[step, side],
            device_id=place(target), device_id_type=MESH,
        )

    def start_exchange(step, value):
        sends[step] = value

        @pl.when(me < ndev - 1)
        def _():
            copy_to(step, 0).start()

        @pl.when(me > 0)
        def _():
            copy_to(step, 1).start()

    def finish_exchange(step, value):
        image = dot_split(value, own[...])

        @pl.when(me > 0)
        def _():
            copy_to(step, 0).wait_recv()

        @pl.when(me < ndev - 1)
        def _():
            copy_to(step, 1).wait_recv()

        both = jnp.concatenate([heard[step, 0], heard[step, 1]], axis=1)
        return image + dot_split(both, sides[...])

    own_group = lane // quant == sub_id

    def start_sum(step, products):
        packed = jnp.zeros((nrhs, width), jnp.float32)
        for q, product in enumerate(products):
            total = jnp.sum(product, axis=1, keepdims=True)
            packed = jnp.where(lane % quant == q, total, packed)
        row = jnp.sum(jnp.where(own_group, packed, 0.0), axis=0, keepdims=True)
        gathered[step, me] = row

        def send(k, carry):
            target = lax.rem(me + k, ndev)
            pltpu.make_async_remote_copy(
                src_ref=gathered.at[step, me], dst_ref=gathered.at[step, me],
                send_sem=gsend_sem.at[step], recv_sem=grecv_sem.at[step],
                device_id=place(target), device_id_type=MESH,
            ).start()
            return carry

        lax.fori_loop(1, ndev, send, 0, unroll=ndev <= 64)

    def all_rows(step, sem):
        span = gathered.at[step, pl.ds(0, ndev - 1)]
        return pltpu.make_async_copy(span, span, sem.at[step])

    def finish_sum(step, count):
        all_rows(step, grecv_sem).wait()
        row = jnp.sum(gathered[step], axis=0)
        spread = jnp.where(own_group, jnp.broadcast_to(row, (nrhs, width)), 0.0)
        return [
            jnp.broadcast_to(
                jnp.sum(jnp.where(lane % quant == q, spread, 0.0), axis=1, keepdims=True),
                (nrhs, width),
            )
            for q in range(count)
        ]

    b = b_ref[...]
    start_exchange(0, b)
    zb = dot_split(b, sketch[...])
    image = finish_exchange(0, b)

    vs, ws, zs, ts = [], [], [], []
    vv, vw, ww = {}, {}, {}
    gram, load = {}, {}
    low, mid, diag_inv = {}, {}, {}

    def factor(i):
        for j in range(i):
            value = gram[i, j]
            for k in range(j):
                value = value - low[i, k] * low[j, k]
            low[i, j] = value * diag_inv[j]
        value = gram[i, i]
        right = load[i]
        for k in range(i):
            value = value - low[i, k] * low[i, k]
            right = right - low[i, k] * mid[k]
        diag_inv[i] = lax.rsqrt(value)
        mid[i] = right * diag_inv[i]

    def window(j):
        return range(max(0, j + 1 - WINDOW), j + 1)

    def next_scale(j):
        length_sq = ww[j, j]
        for i in window(j):
            length_sq = length_sq - 2.0 * vw[i, j] * vw[i, j]
            for k in window(j):
                length_sq = length_sq + vw[i, j] * vv[i, k] * vw[k, j]
        return lax.rsqrt(length_sq)

    def reduced(j, scale, value, parts):
        for i in window(j):
            value = value - vw[i, j] * parts[i]
        return value * scale

    def next_tables(j, scale, vt, wt, tt):
        n = j + 1
        for i in range(n):
            vv[i, n] = vv[n, i] = reduced(j, scale, vw[i, j], [vv[i, k] for k in range(n)])
            vw[i, n] = reduced(j, scale, vt[i], [vw[i, k] for k in range(n)])
            vw[n, i] = reduced(j, scale, ww[j, i], [vw[k, i] for k in range(n)])
            ww[i, n] = reduced(j, scale, wt[i], [ww[i, k] for k in range(n)])
            ww[n, i] = ww[i, n]
        vv[n, n] = one
        vw[n, n] = reduced(j, scale, ww[j, n], [vw[k, n] for k in range(n)])
        square = tt
        for i in window(j):
            square = square - 2.0 * vw[i, j] * wt[i]
            for k in window(j):
                square = square + vw[i, j] * ww[i, k] * vw[k, j]
        ww[n, n] = square * scale * scale

    one = jnp.ones((nrhs, width), jnp.float32)

    x1 = image
    start_exchange(1, x1)
    start_sum(0, [b * b, b * x1, x1 * x1])
    raw_z1 = dot_split(x1, sketch[...])
    x2 = finish_exchange(1, x1)

    start_exchange(2, x2)
    start_sum(1, [b * x2, x1 * x2, x2 * x2, raw_z1 * raw_z1, raw_z1 * zb])
    bb, by, yy = finish_sum(0, 3)
    inv_sq = 1.0 / bb
    inv = lax.rsqrt(bb)
    vs.append(b * inv)
    ws.append(x1 * inv)
    zs.append(raw_z1 * inv)
    ts.append(x2 * inv)
    vv[0, 0], vw[0, 0], ww[0, 0] = one, by * inv_sq, yy * inv_sq
    scale = next_scale(0)
    vs.append(reduced(0, scale, ws[0], vs))
    ws.append(reduced(0, scale, ts[0], ws))
    zs.append(dot_split(ws[1], sketch[...]))
    x3 = finish_exchange(2, x2)
    ts.append(reduced(0, scale, x3 * inv, ts))

    def finish_scaled(j, unit_sq, unit):
        sums = finish_sum(j, 3 * j + 2)
        sums = [value * unit_sq for value in sums[:-1]] + [sums[-1] * unit] if j == 1 else sums
        for i in range(j):
            gram[j - 1, i] = sums[2 * j + 1 + i]
        load[j - 1] = sums[3 * j + 1]
        return sums[:j], sums[j : 2 * j], sums[2 * j]

    for j in range(2, ITERS - 1):
        t = ts[j - 1]
        start_exchange(j + 1, t)
        products = [v * t for v in vs] + [w * t for w in ws] + [t * t]
        start_sum(j, products + [zs[j - 1] * z for z in zs] + [zs[j - 1] * zb])
        next_tables(j - 2, scale, *finish_scaled(j - 1, inv_sq, inv))
        scale = next_scale(j - 1)
        vs.append(reduced(j - 1, scale, ws[j - 1], vs))
        ws.append(reduced(j - 1, scale, t, ws))
        zs.append(dot_split(ws[j], sketch[...]))
        image = finish_exchange(j + 1, t)
        ts.append(reduced(j - 1, scale, image, ts))

    j = ITERS - 1
    t = ts[j - 1]
    fresh = dot_split(t, sketch[...])
    products = [zs[j - 1] * z for z in zs] + [zs[j - 1] * zb]
    products += [fresh * z for z in zs] + [fresh * zb, fresh * fresh]
    start_sum(j, products)
    next_tables(j - 2, scale, *finish_scaled(j - 1, inv_sq, inv))
    scale = next_scale(j - 1)
    vs.append(reduced(j - 1, scale, ws[j - 1], vs))
    ws.append(reduced(j - 1, scale, t, ws))
    for i in range(j - 1):
        factor(i)
    for i in range(ITERS):
        out_ref[2 + i] = vs[i] * math.sqrt(order_total)
    sums = finish_sum(j, len(products))
    for i in range(j):
        gram[j - 1, i] = gram[i, j - 1] = sums[i]
    for i in range(j - 1):
        for k in range(i):
            gram[k, i] = gram[i, k]
    load[j - 1] = sums[j]
    mixed = sums[j + 1 : 2 * j + 1]
    for i in range(j):
        gram[j, i] = reduced(j - 1, scale, mixed[i], [gram[i, k] for k in range(j)])
    load[j] = reduced(j - 1, scale, sums[2 * j + 1], load)
    square = sums[2 * j + 2]
    for i in window(j - 1):
        square = square - 2.0 * vw[i, j - 1] * mixed[i]
        for k in window(j - 1):
            square = square + vw[i, j - 1] * gram[i, k] * vw[k, j - 1]
    gram[j, j] = square * scale * scale
    factor(j - 1)
    factor(j)

    coef = {}
    for i in reversed(range(ITERS)):
        value = mid[i]
        for k in range(i + 1, ITERS):
            value = value - low[k, i] * coef[k]
        coef[i] = value * diag_inv[i]
    answer = coef[0] * vs[0]
    left_over = b - coef[0] * ws[0]
    for i in range(1, ITERS):
        answer = answer + coef[i] * vs[i]
        left_over = left_over - coef[i] * ws[i]
    out_ref[0] = answer
    out_ref[1] = left_over

    for step in range(ITERS):
        all_rows(step, gsend_sem).wait()

        @pl.when(me < ndev - 1)
        def _():
            copy_to(step, 0).wait_send()

        @pl.when(me > 0)
        def _():
            copy_to(step, 1).wait_send()


def deliver(packed_ref, sol_hbm, res_hbm, basis_hbm, sem):
    copies = [
        pltpu.make_async_copy(packed_ref.at[0], sol_hbm, sem.at[0]),
        pltpu.make_async_copy(packed_ref.at[1], res_hbm, sem.at[1]),
        pltpu.make_async_copy(packed_ref.at[pl.ds(2, ITERS)], basis_hbm, sem.at[2]),
    ]
    for copy in copies:
        copy.start()
    for copy in copies:
        copy.wait()


def per_device(ndev, nsub, right_side, matrix_blocks, block_cols, signs, sample_rows):
    nrhs, rows_dev, width = right_side.shape
    nnz = matrix_blocks.shape[1]
    order_total = ndev * rows_dev * width
    vmem = pl.BlockSpec(memory_space=pltpu.VMEM)
    anywhere = pl.BlockSpec(memory_space=pl.ANY)
    listed = sample_rows.shape[0] // width
    packed = pl.pallas_call(
        functools.partial(kernel, ndev, nsub, order_total),
        out_shape=pltpu.VMEM((ITERS + 2, nrhs, width), jnp.float32),
        in_specs=[
            anywhere, anywhere,
            pl.BlockSpec(memory_space=pltpu.SMEM),
            anywhere, anywhere, anywhere,
        ],
        out_specs=vmem,
        scratch_shapes=[
            pltpu.VMEM((nrhs, width), jnp.float32),
            pltpu.VMEM((1, width), jnp.int32),
            pltpu.VMEM((listed, width), jnp.int32),
            pltpu.VMEM((width, width), jnp.float32),
            pltpu.VMEM((nnz, width, width), jnp.float32),
            pltpu.VMEM((3, width, width), jnp.float32),
            pltpu.VMEM((PARTS * width, width), jnp.bfloat16),
            pltpu.VMEM((PARTS * width, 2 * width), jnp.bfloat16),
            pltpu.VMEM((PARTS * width, width), jnp.bfloat16),
            pltpu.VMEM((ITERS, nrhs, width), jnp.float32),
            pltpu.VMEM((ITERS, 2, nrhs, width), jnp.float32),
            pltpu.VMEM((ITERS, ndev, 1, width), jnp.float32),
            pltpu.SemaphoreType.DMA((3,)),
            pltpu.SemaphoreType.DMA((4,)),
            pltpu.SemaphoreType.DMA((ITERS, 2)),
            pltpu.SemaphoreType.DMA((ITERS, 2)),
            pltpu.SemaphoreType.DMA((ITERS,)),
            pltpu.SemaphoreType.DMA((ITERS,)),
        ],
        compiler_params=pltpu.CompilerParams(collective_id=0, has_side_effects=True),
    )(
        right_side.reshape(nrhs, width),
        matrix_blocks.reshape(nnz, width, width),
        block_cols,
        signs,
        sample_rows.reshape(-1, width),
        jnp.asarray(dct_table(width)),
    )
    answer, left_over, basis = pl.pallas_call(
        deliver,
        out_shape=(
            jax.ShapeDtypeStruct((nrhs, width), jnp.float32),
            jax.ShapeDtypeStruct((nrhs, width), jnp.float32),
            jax.ShapeDtypeStruct((ITERS, nrhs, width), jnp.float32),
        ),
        in_specs=[vmem],
        out_specs=(anywhere, anywhere, anywhere),
        scratch_shapes=[pltpu.SemaphoreType.DMA((3,))],
    )(pltpu.with_memory_space_constraint(packed, pltpu.VMEM))
    return (
        answer.reshape(nrhs, rows_dev, width),
        left_over.reshape(nrhs, rows_dev, width),
        basis.reshape(ITERS, nrhs, rows_dev, width),
    )


def solution(mesh):
    nsub = mesh.shape["sub"]
    ndev = mesh.shape["dom"] * nsub
    return jax.shard_map(
        functools.partial(per_device, ndev, nsub),
        mesh=mesh,
        in_specs=(
            P(None, ("dom", "sub"), None),
            P(("dom", "sub"), None, None, None),
            P(("dom", "sub"), None),
            P(("dom", "sub"), None),
            P(),
        ),
        out_specs=(
            P(None, ("dom", "sub"), None),
            P(None, ("dom", "sub"), None),
            P(None, None, ("dom", "sub"), None),
        ),
        check_vma=False,
    )
```
